32 devices in a mesh: unit: 4 (over z), zero: 2 (over x), tp: 4 (over y, core).
Axes of the slice: x: 2, y: 2, z: 4, core: 2. Of those that a mesh axis runs over, the one named last changes fastest.
Arguments:
- weight_query: bfloat16 [16384, 4096], P(('unit', 'zero'), 'tp'), parts along dimension 0, may hold values from -0.125 to 0.125
- low_query: bfloat16 [16384, 32], P(('unit', 'zero')), parts along dimension 0, may hold values from -0.09375 to 0.09375
- high_query: bfloat16 [128, 4096], P('unit', 'tp'), parts along dimension 0, may hold values from -1 to 1
- weight_key: bfloat16 [16384, 1024], P(('unit', 'zero'), 'tp'), parts along dimension 0, may hold values from -0.125 to 0.125
- low_key: bfloat16 [16384, 32], P(('unit', 'zero')), parts along dimension 0, may hold values from -0.09375 to 0.09375
- high_key: bfloat16 [128, 1024], P('unit', 'tp'), parts along dimension 0, may hold values from -1 to 1
- weight_value: bfloat16 [16384, 1024], P(('unit', 'zero'), 'tp'), parts along dimension 0, may hold values from -0.125 to 0.125
- low_value: bfloat16 [16384, 32], P(('unit', 'zero')), parts along dimension 0, may hold values from -0.09375 to 0.09375
- high_value: bfloat16 [128, 1024], P('unit', 'tp'), parts along dimension 0, may hold values from -1 to 1
- norm_train: float32 [16384], P(('unit', 'zero', 'tp')), parts along dimension 0, may hold values from 0.25 to 1.75
- norm_step: float32 [16384], P(('unit', 'zero', 'tp')), parts along dimension 0, may hold values from -0.3 to 0.3
Outputs:
- serve_query: bfloat16 [16384, 4096], P('unit', 'tp'), parts along dimension 0
- serve_key: bfloat16 [16384, 1024], P('unit', 'tp'), parts along dimension 0
- serve_value: bfloat16 [16384, 1024], P('unit', 'tp'), parts along dimension 0
- column_query: float32 [16384], P(('unit', 'tp')), parts along dimension 0
- column_key: float32 [4096], P(('unit', 'tp')), parts along dimension 0
- column_value: float32 [4096], P(('unit', 'tp')), parts along dimension 0
- serve_norm: bfloat16 [16384], P('unit'), parts along dimension 0
The draws below stay inside these ranges and needn't reach their ends.
There are 4 independent parts, one for each index of `unit`. The reference program is written for one: setup_inputs(seed, part) draws one part's arguments, and reference() takes and returns one part's arrays. A program takes and returns all parts, laid end to end along the dimension named above; each array names one. Nothing has to cross between parts.
All inputs are finite; a program needn't handle non-finite values.
Results may differ from the reference program's by a relative error of at most 0.001.
Values may be sent and summed in bfloat16 or wider, within the bound.
A program may use at most 64 MiB of HBM per device.

```python
import jax
import jax.numpy as jnp
from jax import lax

D_MODEL = 4096
Q_DIM = 4096
KV_DIM = 1024
RANK = 32


def spiked(drawn, key, source, target, shards_of, factor):
    owner, partner = [(jnp.arange(drawn.shape[dim]) // (drawn.shape[dim] // shards_of)).reshape([-1 if axis == dim else 1 for axis in range(drawn.ndim)]) for dim in (source, target)]
    chosen = jax.random.permutation(key, shards_of)[partner]
    strong = (owner == chosen) | (owner == (partner + shards_of // 2) % shards_of)
    return jnp.where(strong, factor * drawn, drawn)


def block_levels(stream_key, shape, split, smallest, largest):
    loudness = 1.0
    for position, parts in split:
        draws = jax.random.uniform(jax.random.fold_in(jax.random.fold_in(stream_key, 6), position), (parts,), jnp.float32, smallest / len(split), largest / len(split))
        loudness = loudness * jnp.repeat(jnp.exp(draws), shape[position] // parts).reshape((-1,) + (1,) * (len(shape) - 1 - position))
    return loudness


def centred(stream_key, dims, spread, most, pieces=(), kind=jnp.bfloat16):
    entries = jax.random.normal(stream_key, dims, jnp.float32) * spread
    if len(pieces) > 0:
        entries = block_levels(stream_key, dims, pieces, -0.22, 0.18) * entries
    return jnp.clip(entries, min=-most, max=most).astype(kind)


def gaussian_with(rng, extent, scale, reach, shards, heavy, kind=jnp.bfloat16):
    result = scale * jax.random.normal(rng, extent, jnp.float32)
    if shards:
        result = result * block_levels(rng, extent, shards, -0.22, 0.18)
    return jnp.clip(spiked(result, jax.random.fold_in(rng, 3), *heavy), -reach, reach).astype(kind)


def setup_inputs(seed: int = 0, part: int = 0) -> dict:
    streams_of = jax.random.split(jax.random.key(seed), 12)
    part_splits = jax.random.split(jax.random.fold_in(streams_of[11], part), 12)
    weight_query = gaussian_with(part_splits[0], (D_MODEL, Q_DIM), D_MODEL ** -0.5, 0.125, ((0, 2), (1, 4)), (0, 1, 4, 2.0))
    low_query = centred(part_splits[1], (D_MODEL, RANK), D_MODEL ** -0.5, 0.09375, ((0, 2),))
    high_query = centred(part_splits[2], (RANK, Q_DIM), RANK ** -0.5, 1.0, ((1, 4),))
    weight_key = gaussian_with(part_splits[3], (D_MODEL, KV_DIM), D_MODEL ** -0.5, 0.125, ((0, 2), (1, 4)), (0, 1, 4, 2.0))
    low_key = centred(part_splits[4], (D_MODEL, RANK), D_MODEL ** -0.5, 0.09375, ((0, 2),))
    high_key = centred(part_splits[5], (RANK, KV_DIM), RANK ** -0.5, 1.0, ((1, 4),))
    weight_value = gaussian_with(part_splits[6], (D_MODEL, KV_DIM), D_MODEL ** -0.5, 0.125, ((0, 2), (1, 4)), (0, 1, 4, 2.0))
    low_value = centred(part_splits[7], (D_MODEL, RANK), D_MODEL ** -0.5, 0.09375, ((0, 2),))
    high_value = centred(part_splits[8], (RANK, KV_DIM), RANK ** -0.5, 1.0, ((1, 4),))
    norm_train = jnp.clip(1.0 + 0.15 * jax.random.normal(part_splits[9], (D_MODEL,), jnp.float32), 0.25, 1.75)
    norm_step = jnp.clip(jax.random.uniform(part_splits[10], (D_MODEL,), jnp.float32, -0.3, 0.3) * block_levels(part_splits[10], (D_MODEL,), ((0, 8),), -0.4, 0.0), -0.3, 0.3)
    return dict(weight_query=weight_query, low_query=low_query, high_query=high_query, weight_key=weight_key, low_key=low_key, high_key=high_key, weight_value=weight_value, low_value=low_value, high_value=high_value, norm_train=norm_train, norm_step=norm_step)


mix_rate = 2.0

def reference(weight_query, low_query, high_query, weight_key, low_key, high_key, weight_value, low_value, high_value, norm_train, norm_step):
    fresh_query = weight_query.astype(jnp.float32) + mix_rate * jnp.dot(low_query, high_query, preferred_element_type=jnp.float32)
    fresh_key = weight_key.astype(jnp.float32) + mix_rate * jnp.dot(low_key, high_key, preferred_element_type=jnp.float32)
    fresh_value = weight_value.astype(jnp.float32) + mix_rate * jnp.dot(low_value, high_value, preferred_element_type=jnp.float32)
    column_query = jnp.sqrt(lax.optimization_barrier(jnp.sum(fresh_query * fresh_query, axis=0)))
    serve_query = (fresh_query / column_query).astype(jnp.bfloat16)
    column_key = jnp.sqrt(lax.optimization_barrier(jnp.sum(fresh_key * fresh_key, axis=0)))
    serve_key = (fresh_key / column_key).astype(jnp.bfloat16)
    column_value = jnp.sqrt(lax.optimization_barrier(jnp.sum(fresh_value * fresh_value, axis=0)))
    serve_value = (fresh_value / column_value).astype(jnp.bfloat16)
    serve_norm = (norm_train + norm_step).astype(jnp.bfloat16)
    return (serve_query, serve_key, serve_value, column_query, column_key, column_value, serve_norm)
```

```python
import functools

import jax
import jax.numpy as jnp
from jax import lax
from jax.experimental import pallas as pl
from jax.experimental.pallas import tpu as pltpu
from jax.sharding import PartitionSpec as P

mix_rate = 2.0


def finish_kernel(n, rows, tile, has_prev, *refs):
    own_ref, others, low_ref, high_ref = refs[0], refs[1:n], refs[n], refs[n + 1]
    out_ref, col_ref, fresh, total = refs[n + 2 + has_prev :]
    me = lax.axis_index("zero")
    total[...] = jnp.zeros_like(total)
    width = out_ref.shape[1]
    for slot, piece in enumerate((own_ref,) + tuple(others)):

        @pl.loop(0, rows // tile)
        def _(t):
            at = pl.multiple_of(t * tile, tile)
            merged = piece[pl.ds(at, tile), :].astype(jnp.float32) + mix_rate * lax.dot_general(
                low_ref[slot, :, pl.ds(at, tile)],
                high_ref[...],
                (((0,), (0,)), ((), ())),
                preferred_element_type=jnp.float32,
            )
            fresh[pl.ds(pl.multiple_of(slot * rows + at, tile), tile), :] = merged
            total[...] += jnp.sum((merged * merged).reshape(tile // 8, 8, width), axis=0)

    column = jnp.sqrt(jnp.sum(total[...], axis=0, keepdims=True))
    col_ref[...] = column
    inverse = 1.0 / column
    for slot in range(n):
        owner = lax.rem(me + n - slot, n)

        @pl.loop(0, rows // tile)
        def _(t):
            at = pl.multiple_of(t * tile, tile)
            out_ref[pl.ds(pl.multiple_of(owner * rows + at, tile), tile), :] = (
                fresh[pl.ds(pl.multiple_of(slot * rows + at, tile), tile), :] * inverse
            ).astype(out_ref.dtype)


def finish(n, weight, others, low, high, start, width, prev):
    rows, full = weight.shape
    rank = high.shape[0]
    block = start // width
    tile = min(rows, 256)
    args = [weight, *others, low, high]
    specs = (
        [pl.BlockSpec((rows, width), lambda i: (0, block))]
        + [pl.BlockSpec((rows, width), lambda i: (0, 0))] * (n - 1)
        + [
            pl.BlockSpec((n, rank, rows), lambda i: (0, 0, 0)),
            pl.BlockSpec((rank, width), lambda i: (0, block)),
        ]
    )
    alias = {}
    if prev is not None:
        args.append(prev)
        specs.append(pl.BlockSpec(memory_space=pl.ANY))
        alias = {len(args) - 1: 0}
    elements = n * rows * width
    return pl.pallas_call(
        functools.partial(finish_kernel, n, rows, tile, int(prev is not None)),
        grid=(1,),
        out_shape=(
            jax.ShapeDtypeStruct((n * rows, full), jnp.bfloat16),
            jax.ShapeDtypeStruct((1, width), jnp.float32),
        ),
        in_specs=specs,
        out_specs=(
            pl.BlockSpec((n * rows, width), lambda i: (0, block)),
            pl.BlockSpec((1, width), lambda i: (0, 0)),
        ),
        scratch_shapes=[
            pltpu.VMEM((n * rows, width), jnp.float32),
            pltpu.VMEM((8, width), jnp.float32),
        ],
        input_output_aliases=alias,
        cost_estimate=pl.CostEstimate(
            flops=2 * elements * rank, bytes_accessed=8 * elements, transcendentals=0
        ),
    )(*args)


def on_device(
    n,
    parts,
    weight_query,
    low_query,
    high_query,
    weight_key,
    low_key,
    high_key,
    weight_value,
    low_value,
    high_value,
    norm_train,
    norm_step,
):
    rows = weight_query.shape[0]
    rank = high_query.shape[0]
    me, tp = lax.axis_index("zero"), lax.axis_index("tp")

    def shifted(array):
        return [
            lax.ppermute(array, "zero", [(i, (i + k) % n) for i in range(n)]) for k in range(1, n)
        ]

    def cut(width):
        big = min(256, width)
        starts = [(s, big) for s in range(0, width, big)]
        s, w = starts[-1]
        if width > big and w % 256 == 0:
            starts[-1:] = [(s, w // 2), (s + w // 2, w // 2)]
        return starts

    value_parts = shifted(weight_value)

    piece = rows // parts
    lows = [
        lax.dynamic_slice(low, (tp * piece, 0), (piece, rank)).T
        for low in (low_query, low_key, low_value)
    ]
    norm = (norm_train + norm_step).astype(jnp.bfloat16)
    packed = jnp.concatenate(lows + [norm.reshape(-1, piece)], axis=0)
    packs = jnp.stack([packed] + shifted(packed))
    packs = lax.all_gather(packs, "tp", axis=2, tiled=True)
    low_all = packs[:, : 3 * rank]
    gain = packs[:, 3 * rank :].reshape(n, -1, parts, piece)
    gain = jnp.swapaxes(gain, 1, 2).reshape(n, -1)
    serve_norm = jnp.zeros_like(gain)
    for slot in range(n):
        serve_norm = lax.dynamic_update_slice(
            serve_norm, gain[slot : slot + 1], ((me + n - slot) % n, 0)
        )
    serve_norm = serve_norm.reshape(-1)

    key_parts = shifted(weight_key)
    serve_value, column_value = finish(
        n, weight_value, value_parts, low_all[:, 2 * rank :], high_value, 0, weight_value.shape[1], None
    )
    serve_key, column_key = finish(
        n, weight_key, key_parts, low_all[:, rank : 2 * rank], high_key, 0, weight_key.shape[1], None
    )
    serve_query, columns = None, []
    for start, width in cut(weight_query.shape[1]):
        others = shifted(weight_query[:, start : start + width])
        serve_query, column = finish(
            n, weight_query, others, low_all[:, :rank], high_query, start, width, serve_query
        )
        columns.append(column)
    column_query = jnp.concatenate(columns, axis=1)
    return (
        serve_query,
        serve_key,
        serve_value,
        column_query.reshape(-1),
        column_key.reshape(-1),
        column_value.reshape(-1),
        serve_norm,
    )


def solution(mesh):
    placed = (
        P(("unit", "zero"), "tp"),
        P(("unit", "zero"), None),
        P("unit", "tp"),
        P(("unit", "zero"), "tp"),
        P(("unit", "zero"), None),
        P("unit", "tp"),
        P(("unit", "zero"), "tp"),
        P(("unit", "zero"), None),
        P("unit", "tp"),
        P(("unit", "zero", "tp")),
        P(("unit", "zero", "tp")),
    )
    return jax.shard_map(
        functools.partial(on_device, mesh.shape["zero"], mesh.shape["tp"]),
        mesh=mesh,
        in_specs=placed,
        out_specs=(
            P("unit", "tp"),
            P("unit", "tp"),
            P("unit", "tp"),
            P(("unit", "tp")),
            P(("unit", "tp")),
            P(("unit", "tp")),
            P("unit"),
        ),
        check_vma=False,
    )
```

```python
import functools

import jax
import jax.numpy as jnp
from jax import lax
from jax.experimental import pallas as pl
from jax.experimental.pallas import tpu as pltpu
from jax.sharding import PartitionSpec as P

mix_rate = 2.0


def finish_kernel(n, rows, tile, extra, *refs):
    own_ref, others, low_ref, high_ref = refs[0], refs[1:n], refs[n], refs[n + 1]
    out_ref, col_ref, fresh, total = refs[n + 2 + extra :]
    me = lax.axis_index("zero")
    total[...] = jnp.zeros_like(total)
    width = out_ref.shape[1]
    for slot, piece in enumerate((own_ref,) + tuple(others)):

        @pl.loop(0, rows // tile)
        def _(t):
            at = pl.multiple_of(t * tile, tile)
            merged = piece[pl.ds(at, tile), :].astype(jnp.float32) + mix_rate * lax.dot_general(
                low_ref[slot, pl.ds(at, tile), :],
                high_ref[...],
                (((1,), (0,)), ((), ())),
                preferred_element_type=jnp.float32,
            )
            fresh[pl.ds(pl.multiple_of(slot * rows + at, tile), tile), :] = merged
            total[...] += jnp.sum((merged * merged).reshape(tile // 8, 8, width), axis=0)

    column = jnp.sqrt(jnp.sum(total[...], axis=0, keepdims=True))
    col_ref[...] = column
    inverse = 1.0 / column
    for slot in range(n):
        owner = lax.rem(me + n - slot, n)

        @pl.loop(0, rows // tile)
        def _(t):
            at = pl.multiple_of(t * tile, tile)
            out_ref[pl.ds(pl.multiple_of(owner * rows + at, tile), tile), :] = (
                fresh[pl.ds(pl.multiple_of(slot * rows + at, tile), tile), :] * inverse
            ).astype(out_ref.dtype)


def finish(n, weight, others, low, high, start, width, prev, after):
    rows, full = weight.shape
    rank = high.shape[0]
    block = start // width
    tile = min(rows, 256)
    args = [weight, *others, low, high]
    specs = (
        [pl.BlockSpec((rows, width), lambda i: (0, block))]
        + [pl.BlockSpec((rows, width), lambda i: (0, 0))] * (n - 1)
        + [
            pl.BlockSpec((n, rows, rank), lambda i: (0, 0, 0)),
            pl.BlockSpec((rank, width), lambda i: (0, block)),
        ]
    )
    alias = {}
    if prev is not None:
        alias = {len(args): 0, len(args) + 1: 1}
        args += prev
    elif after is not None:
        args.append(after)
    extra = len(args) - len(specs)
    specs += [pl.BlockSpec(memory_space=pl.ANY)] * extra
    elements = n * rows * width
    return pl.pallas_call(
        functools.partial(finish_kernel, n, rows, tile, extra),
        grid=(1,),
        out_shape=(
            jax.ShapeDtypeStruct((n * rows, full), jnp.bfloat16),
            jax.ShapeDtypeStruct((1, full), jnp.float32),
        ),
        in_specs=specs,
        out_specs=(
            pl.BlockSpec((n * rows, width), lambda i: (0, block)),
            pl.BlockSpec((1, width), lambda i: (0, block)),
        ),
        scratch_shapes=[
            pltpu.VMEM((n * rows, width), jnp.float32),
            pltpu.VMEM((8, width), jnp.float32),
        ],
        input_output_aliases=alias,
        cost_estimate=pl.CostEstimate(
            flops=2 * elements * rank, bytes_accessed=8 * elements, transcendentals=0
        ),
    )(*args)


def prepare_kernel(n, rows, tile, own_ref, low_ref, high_ref, fresh_ref, delta_ref, total_ref):
    width = fresh_ref.shape[1]
    total_ref[...] = jnp.zeros_like(total_ref)
    for slot in range(n):

        @pl.loop(0, rows // tile)
        def _(t):
            at = pl.multiple_of(t * tile, tile)
            added = mix_rate * jnp.dot(
                low_ref[slot, pl.ds(at, tile), :],
                high_ref[...],
                preferred_element_type=jnp.float32,
            )
            if slot == 0:
                merged = own_ref[pl.ds(at, tile), :].astype(jnp.float32) + added
                fresh_ref[pl.ds(at, tile), :] = merged
                total_ref[...] += jnp.sum((merged * merged).reshape(tile // 8, 8, width), axis=0)
            else:
                delta_ref[slot - 1, pl.ds(at, tile), :] = added


def last_kernel(n, rows, pieces, start, *refs):
    others, own_hbm, delta_hbm, total_ref = refs[: n - 1], refs[n - 1], refs[n], refs[n + 1]
    out_hbm, col_hbm, raw, own, delta, done, norms = refs[n + 4 : n + 11]
    raw_sem, delta_sem, own_sem, out_sem, norm_sem = refs[n + 11 :]
    me = lax.axis_index("zero")
    width = own.shape[1]
    size = rows // pieces
    tile = min(size, 128)
    loads, adds, stores = [], [], []
    for slot in range(n - 1):
        for p in range(pieces):
            at = pl.ds(p * size, size)
            loads.append(pltpu.make_async_copy(others[slot].at[at], raw.at[slot, at], raw_sem.at[slot, p]))
            adds.append(
                pltpu.make_async_copy(delta_hbm.at[slot, at], delta.at[slot, at], delta_sem.at[slot, p])
            )
    for load, add in zip(loads, adds):
        load.start()
        add.start()
    fetch = pltpu.make_async_copy(own_hbm, own, own_sem)
    fetch.start()
    sums = total_ref[...]
    for slot in range(n - 1):
        for p in range(pieces):
            loads[slot * pieces + p].wait()
            adds[slot * pieces + p].wait()
            for t in range(size // tile):
                at = pl.ds(p * size + t * tile, tile)
                merged = raw[slot, at, :].astype(jnp.float32) + delta[slot, at, :]
                delta[slot, at, :] = merged
                sums += jnp.sum((merged * merged).reshape(tile // 8, 8, width), axis=0)
    column = jnp.sqrt(jnp.sum(sums, axis=0, keepdims=True))
    norms[...] = column
    inverse = 1.0 / column
    stores.append(pltpu.make_async_copy(norms, col_hbm.at[:, pl.ds(start, width)], norm_sem))
    stores[0].start()
    fetch.wait()
    for slot in range(n):
        owner = lax.rem(me + n - slot, n)
        for p in range(pieces):
            for t in range(size // tile):
                at = pl.ds(p * size + t * tile, tile)
                merged = own[at, :] if slot == 0 else delta[slot - 1, at, :]
                done[slot, at, :] = (merged * inverse).astype(done.dtype)
            store = pltpu.make_async_copy(
                done.at[slot, pl.ds(p * size, size)],
                out_hbm.at[
                    pl.ds(pl.multiple_of(owner * rows + p * size, size), size), pl.ds(start, width)
                ],
                out_sem.at[slot, p],
            )
            store.start()
            stores.append(store)
    for store in stores:
        store.wait()


def finish_last(n, weight, others, low, high, start, width, prev, after):
    rows, full = weight.shape
    rank = high.shape[0]
    block = start // width
    pieces = max(1, min(4, rows // 256))
    elements = n * rows * width
    fresh, delta, total = pl.pallas_call(
        functools.partial(prepare_kernel, n, rows, min(rows, 256)),
        grid=(1,),
        out_shape=(
            jax.ShapeDtypeStruct((rows, width), jnp.float32),
            jax.ShapeDtypeStruct((n - 1, rows, width), jnp.float32),
            jax.ShapeDtypeStruct((8, width), jnp.float32),
        ),
        in_specs=[
            pl.BlockSpec((rows, width), lambda i: (0, block)),
            pl.BlockSpec((n, rows, rank), lambda i: (0, 0, 0)),
            pl.BlockSpec((rank, width), lambda i: (0, block)),
        ],
        out_specs=(
            pl.BlockSpec((rows, width), lambda i: (0, 0)),
            pl.BlockSpec((n - 1, rows, width), lambda i: (0, 0, 0)),
            pl.BlockSpec((8, width), lambda i: (0, 0)),
        ),
        name="prepare",
        cost_estimate=pl.CostEstimate(
            flops=2 * elements * rank, bytes_accessed=8 * elements, transcendentals=0
        ),
    )(weight, low, high)
    hbm, vmem = pl.BlockSpec(memory_space=pl.ANY), pl.BlockSpec(memory_space=pltpu.VMEM)
    return pl.pallas_call(
        functools.partial(last_kernel, n, rows, pieces, start),
        out_shape=(
            jax.ShapeDtypeStruct((n * rows, full), jnp.bfloat16),
            jax.ShapeDtypeStruct((1, full), jnp.float32),
        ),
        in_specs=[hbm] * (n - 1) + [hbm, hbm, vmem, hbm, hbm],
        out_specs=(hbm, hbm),
        scratch_shapes=[
            pltpu.VMEM((n - 1, rows, width), jnp.bfloat16),
            pltpu.VMEM((rows, width), jnp.float32),
            pltpu.VMEM((n - 1, rows, width), jnp.float32),
            pltpu.VMEM((n, rows, width), jnp.bfloat16),
            pltpu.VMEM((1, width), jnp.float32),
            pltpu.SemaphoreType.DMA((n - 1, pieces)),
            pltpu.SemaphoreType.DMA((n - 1, pieces)),
            pltpu.SemaphoreType.DMA,
            pltpu.SemaphoreType.DMA((n, pieces)),
            pltpu.SemaphoreType.DMA,
        ],
        input_output_aliases={n + 2: 0, n + 3: 1},
        name="last",
        cost_estimate=pl.CostEstimate(
            flops=4 * elements, bytes_accessed=8 * elements, transcendentals=0
        ),
    )(*others, fresh, delta, total, *prev)


def on_device(
    n,
    parts,
    weight_query,
    low_query,
    high_query,
    weight_key,
    low_key,
    high_key,
    weight_value,
    low_value,
    high_value,
    norm_train,
    norm_step,
):
    rows = weight_query.shape[0]
    rank = high_query.shape[0]
    me, tp = lax.axis_index("zero"), lax.axis_index("tp")

    def shifted(array):
        return [
            lax.ppermute(array, "zero", [(i, (i + k) % n) for i in range(n)])
            for k in range(1, n)
        ]

    def cut(width):
        big = min(256, width)
        starts = [(s, big) for s in range(0, width, big)]
        s, w = starts[-1]
        if width > big and w % 256 == 0:
            starts[-1:] = [(s, w // 2), (s + w // 2, w // 2)]
        return starts

    value_parts = shifted(weight_value)

    piece = rows // parts
    lows = [
        lax.dynamic_slice(low, (tp * piece, 0), (piece, rank)).T
        for low in (low_query, low_key, low_value)
    ]
    norm = (norm_train + norm_step).astype(jnp.bfloat16)
    packed = jnp.concatenate(lows + [norm.reshape(-1, piece)], axis=0)
    packs = jnp.stack([packed] + shifted(packed))
    packs = lax.all_gather(packs, "tp", axis=2, tiled=True)
    low_all = jnp.swapaxes(packs[:, : 3 * rank], 1, 2)
    gain = packs[:, 3 * rank :].reshape(n, -1, parts, piece)
    gain = jnp.swapaxes(gain, 1, 2).reshape(n, -1)
    serve_norm = jnp.zeros_like(gain)
    for slot in range(n):
        serve_norm = lax.dynamic_update_slice(
            serve_norm, gain[slot : slot + 1], ((me + n - slot) % n, 0)
        )
    serve_norm = serve_norm.reshape(-1)

    key_parts = shifted(weight_key)
    serve_value, column_value = finish(
        n, weight_value, value_parts, low_all[:, :, 2 * rank :], high_value, 0, weight_value.shape[1], None, None
    )
    serve_key, column_key = finish(
        n, weight_key, key_parts, low_all[:, :, rank : 2 * rank], high_key, 0, weight_key.shape[1], None, column_value
    )
    done = None
    chunks = cut(weight_query.shape[1])
    for number, (start, width) in enumerate(chunks):
        sent = weight_query[:, start : start + width]
        others = shifted(sent)
        step = finish_last if n > 1 and 0 < number == len(chunks) - 1 else finish
        done = step(
            n, weight_query, others, low_all[:, :, :rank], high_query, start, width, done, column_key
        )
    serve_query, column_query = done
    return (
        serve_query,
        serve_key,
        serve_value,
        column_query.reshape(-1),
        column_key.reshape(-1),
        column_value.reshape(-1),
        serve_norm,
    )


def solution(mesh):
    placed = (
        P(("unit", "zero"), "tp"),
        P(("unit", "zero"), None),
        P("unit", "tp"),
        P(("unit", "zero"), "tp"),
        P(("unit", "zero"), None),
        P("unit", "tp"),
        P(("unit", "zero"), "tp"),
        P(("unit", "zero"), None),
        P("unit", "tp"),
        P(("unit", "zero", "tp")),
        P(("unit", "zero", "tp")),
    )

    def body(*args):
        return on_device(mesh.shape["zero"], mesh.shape["tp"], *args)

    return jax.shard_map(
        body,
        mesh=mesh,
        in_specs=placed,
        out_specs=(
            P("unit", "tp"),
            P("unit", "tp"),
            P("unit", "tp"),
            P(("unit", "tp")),
            P(("unit", "tp")),
            P(("unit", "tp")),
            P("unit"),
        ),
        check_vma=False,
    )
```

```python
import functools

import jax
import jax.numpy as jnp
from jax import lax
from jax.experimental import pallas as pl
from jax.experimental.pallas import tpu as pltpu
from jax.sharding import PartitionSpec as P

mix_rate = 2.0


def finish_kernel(n, rows, tile, extra, *refs):
    own_ref, others, low_ref, high_ref = refs[0], refs[1:n], refs[n], refs[n + 1]
    out_ref, col_ref, fresh, total = refs[n + 2 + extra :]
    me = lax.axis_index("zero")
    total[...] = jnp.zeros_like(total)
    width = out_ref.shape[1]
    for slot, piece in enumerate((own_ref,) + tuple(others)):
        giver = lax.rem(me + n - slot, n)

        @pl.loop(0, rows // tile)
        def _(t):
            at = pl.multiple_of(t * tile, tile)
            merged = piece[pl.ds(at, tile), :].astype(jnp.float32) + mix_rate * lax.dot_general(
                low_ref[slot, pl.ds(at, tile), :],
                high_ref[...],
                (((1,), (0,)), ((), ())),
                preferred_element_type=jnp.float32,
            )
            fresh[pl.ds(pl.multiple_of(slot * rows + at, tile), tile), :] = merged
            total[giver] += jnp.sum((merged * merged).reshape(tile // 8, 8, width), axis=0)

    column = jnp.sqrt(jnp.sum(jnp.sum(total[...], axis=0), axis=0, keepdims=True))
    col_ref[...] = column
    inverse = 1.0 / column
    for slot in range(n):
        owner = lax.rem(me + n - slot, n)

        @pl.loop(0, rows // tile)
        def _(t):
            at = pl.multiple_of(t * tile, tile)
            out_ref[pl.ds(pl.multiple_of(owner * rows + at, tile), tile), :] = (
                fresh[pl.ds(pl.multiple_of(slot * rows + at, tile), tile), :] * inverse
            ).astype(out_ref.dtype)


def finish(n, weight, others, low, high, after):
    rows, width = weight.shape
    rank = high.shape[0]
    tile = min(rows, 256)
    args = [weight, *others, low, high]
    specs = (
        [pl.BlockSpec((rows, width), lambda i: (0, 0))]
        + [pl.BlockSpec((rows, width), lambda i: (0, 0))] * (n - 1)
        + [
            pl.BlockSpec((n, rows, rank), lambda i: (0, 0, 0)),
            pl.BlockSpec((rank, width), lambda i: (0, 0)),
        ]
    )
    if after is not None:
        args.append(after)
    extra = len(args) - len(specs)
    specs += [pl.BlockSpec(memory_space=pl.ANY)] * extra
    elements = n * rows * width
    return pl.pallas_call(
        functools.partial(finish_kernel, n, rows, tile, extra),
        grid=(1,),
        out_shape=(
            jax.ShapeDtypeStruct((n * rows, width), jnp.bfloat16),
            jax.ShapeDtypeStruct((1, width), jnp.float32),
        ),
        in_specs=specs,
        out_specs=(
            pl.BlockSpec((n * rows, width), lambda i: (0, 0)),
            pl.BlockSpec((1, width), lambda i: (0, 0)),
        ),
        scratch_shapes=[
            pltpu.VMEM((n * rows, width), jnp.float32),
            pltpu.VMEM((n, 8, width), jnp.float32),
        ],
        cost_estimate=pl.CostEstimate(
            flops=2 * elements * rank, bytes_accessed=8 * elements, transcendentals=0
        ),
    )(*args)


def merge(piece, low, high):
    return piece.astype(jnp.float32) + mix_rate * jnp.dot(
        low, high, preferred_element_type=jnp.float32
    )


def groups(full):
    wide = min(256, full)
    return [pl.ds(s, wide) for s in range(0, full, wide)]


def sums_kernel(weight_ref, low_ref, high_ref, sum_ref):
    @pl.when(pl.program_id(0) == 0)
    def _():
        sum_ref[...] = jnp.zeros_like(sum_ref)

    for at in groups(sum_ref.shape[1]):
        merged = merge(weight_ref[:, at], low_ref[...], high_ref[:, at])
        sum_ref[:, at] += jnp.sum(merged * merged, axis=0, keepdims=True)


def serve_kernel(weight_ref, low_ref, high_ref, column_ref, out_ref):
    for at in groups(out_ref.shape[1]):
        merged = merge(weight_ref[:, at], low_ref[...], high_ref[:, at])
        out_ref[:, at] = (merged * (1.0 / column_ref[:, at])).astype(out_ref.dtype)


def own_rows(kernel, weight, low, high, column, start, size):
    full, rank = weight.shape[1], high.shape[0]
    tile = min(size, 256)
    first = start // tile
    args = [weight, low, high]
    specs = [
        pl.BlockSpec((tile, full), lambda i: (first + i, 0)),
        pl.BlockSpec((tile, rank), lambda i: (first + i, 0)),
        pl.BlockSpec((rank, full), lambda i: (0, 0)),
    ]
    line = pl.BlockSpec((1, full), lambda i: (0, 0))
    if column is None:
        out_shape, out_spec = jax.ShapeDtypeStruct((1, full), jnp.float32), line
    else:
        args.append(column)
        specs.append(line)
        out_shape = jax.ShapeDtypeStruct((size, full), jnp.bfloat16)
        out_spec = pl.BlockSpec((tile, full), lambda i: (i, 0))
    return pl.pallas_call(
        kernel,
        grid=(size // tile,),
        out_shape=out_shape,
        in_specs=specs,
        out_specs=out_spec,
        cost_estimate=pl.CostEstimate(
            flops=2 * size * full * rank, bytes_accessed=4 * size * full, transcendentals=0
        ),
    )(*args)


def on_device(
    n,
    parts,
    weight_query,
    low_query,
    high_query,
    weight_key,
    low_key,
    high_key,
    weight_value,
    low_value,
    high_value,
    norm_train,
    norm_step,
):
    rows = weight_query.shape[0]
    rank = high_query.shape[0]
    me, tp = lax.axis_index("zero"), lax.axis_index("tp")

    def shifted(array):
        return [
            lax.ppermute(array, "zero", [(i, (i + k) % n) for i in range(n)])
            for k in range(1, n)
        ]

    def in_order(mine, others, axis):
        size = mine.shape[axis]
        shape = list(mine.shape)
        shape[axis] *= n
        whole = jnp.zeros(shape, mine.dtype)
        for slot, piece in enumerate([mine] + list(others)):
            at = [0] * len(shape)
            at[axis] = (me + n - slot) % n * size
            whole = lax.dynamic_update_slice(whole, piece, at)
        return whole

    value_parts = shifted(weight_value)

    piece = rows // parts
    lows = [
        lax.dynamic_slice(low, (tp * piece, 0), (piece, rank)).T
        for low in (low_key, low_value)
    ]
    norm = (norm_train + norm_step).astype(jnp.bfloat16)
    packed = jnp.concatenate(lows + [norm.reshape(-1, piece)], axis=0)
    shape = packed.shape
    if packed.size % 128 == 0:
        packed = packed.reshape(-1, 128)
    sent = shifted(packed)
    total = own_rows(sums_kernel, weight_query, low_query, high_query, None, 0, rows)
    totals = in_order(total, shifted(total), 0)
    column_query = jnp.sqrt(jnp.sum(totals, axis=0, keepdims=True))
    key_parts = shifted(weight_key)

    sizes = [rows // 2, rows // 4, rows // 8, rows // 16]
    sizes.append(rows - sum(sizes))
    mine, theirs, start = [], [], 0
    for size in sizes:
        chunk = own_rows(serve_kernel, weight_query, low_query, high_query, column_query, start, size)
        mine.append((start, chunk))
        theirs.append((start, shifted(chunk)))
        start += size

    packs = jnp.stack([a.reshape(shape) for a in [packed] + sent])
    packs = lax.all_gather(packs, "tp", axis=2, tiled=True)
    low_all = jnp.swapaxes(packs[:, : 2 * rank], 1, 2)
    gain = packs[:, 2 * rank :].reshape(n, -1, parts, piece)
    gain = jnp.swapaxes(gain, 1, 2).reshape(n, -1)
    serve_norm = in_order(gain[:1], [gain[k : k + 1] for k in range(1, n)], 0).reshape(-1)
    serve_value, column_value = finish(
        n, weight_value, value_parts, low_all[:, :, rank:], high_value, None
    )
    serve_key, column_key = finish(
        n, weight_key, key_parts, low_all[:, :, :rank], high_key, column_value
    )
    serve_query = jnp.zeros((n * rows, weight_query.shape[1]), jnp.bfloat16)
    for start, chunk in mine:
        serve_query = lax.dynamic_update_slice(serve_query, chunk, (me * rows + start, 0))
    for start, arrived in theirs:
        for k, chunk in enumerate(arrived):
            owner = (me + n - 1 - k) % n
            serve_query = lax.dynamic_update_slice(serve_query, chunk, (owner * rows + start, 0))
    return (
        serve_query,
        serve_key,
        serve_value,
        column_query.reshape(-1),
        column_key.reshape(-1),
        column_value.reshape(-1),
        serve_norm,
    )


def solution(mesh):
    placed = (
        P(("unit", "zero"), "tp"),
        P(("unit", "zero"), None),
        P("unit", "tp"),
        P(("unit", "zero"), "tp"),
        P(("unit", "zero"), None),
        P("unit", "tp"),
        P(("unit", "zero"), "tp"),
        P(("unit", "zero"), None),
        P("unit", "tp"),
        P(("unit", "zero", "tp")),
        P(("unit", "zero", "tp")),
    )

    def body(*args):
        return on_device(mesh.shape["zero"], mesh.shape["tp"], *args)

    return jax.shard_map(
        body,
        mesh=mesh,
        in_specs=placed,
        out_specs=(
            P("unit", "tp"),
            P("unit", "tp"),
            P("unit", "tp"),
            P(("unit", "tp")),
            P(("unit", "tp")),
            P(("unit", "tp")),
            P("unit"),
        ),
        check_vma=False,
    )
```

```python
import functools

import jax
import jax.numpy as jnp
from jax import lax
from jax.experimental import pallas as pl
from jax.experimental.pallas import tpu as pltpu
from jax.sharding import PartitionSpec as P

mix_rate = 2.0


def finish_kernel(n, rows, tile, extra, *refs):
    own_ref, others, low_ref, high_ref = refs[0], refs[1:n], refs[n], refs[n + 1]
    out_ref, col_ref, fresh, total = refs[n + 2 + extra :]
    me = lax.axis_index("zero")
    total[...] = jnp.zeros_like(total)
    width = out_ref.shape[1]
    for slot, piece in enumerate((own_ref,) + tuple(others)):
        giver = lax.rem(me + n - slot, n)

        @pl.loop(0, rows // tile)
        def _(t):
            at = pl.multiple_of(t * tile, tile)
            merged = piece[pl.ds(at, tile), :].astype(jnp.float32) + mix_rate * lax.dot_general(
                low_ref[slot, pl.ds(at, tile), :],
                high_ref[...],
                (((1,), (0,)), ((), ())),
                preferred_element_type=jnp.float32,
            )
            fresh[pl.ds(pl.multiple_of(slot * rows + at, tile), tile), :] = merged
            total[giver] += jnp.sum((merged * merged).reshape(tile // 8, 8, width), axis=0)

    column = jnp.sqrt(jnp.sum(jnp.sum(total[...], axis=0), axis=0, keepdims=True))
    col_ref[...] = column
    inverse = 1.0 / column
    for slot in range(n):
        owner = lax.rem(me + n - slot, n)

        @pl.loop(0, rows // tile)
        def _(t):
            at = pl.multiple_of(t * tile, tile)
            out_ref[pl.ds(pl.multiple_of(owner * rows + at, tile), tile), :] = (
                fresh[pl.ds(pl.multiple_of(slot * rows + at, tile), tile), :] * inverse
            ).astype(out_ref.dtype)


def finish(n, weight, others, low, high, after):
    rows, width = weight.shape
    rank = high.shape[0]
    tile = min(rows, 256)
    args = [weight, *others, low, high]
    specs = (
        [pl.BlockSpec((rows, width), lambda i: (0, 0))]
        + [pl.BlockSpec((rows, width), lambda i: (0, 0))] * (n - 1)
        + [
            pl.BlockSpec((n, rows, rank), lambda i: (0, 0, 0)),
            pl.BlockSpec((rank, width), lambda i: (0, 0)),
        ]
    )
    if after is not None:
        args.append(after)
    extra = len(args) - len(specs)
    specs += [pl.BlockSpec(memory_space=pl.ANY)] * extra
    elements = n * rows * width
    return pl.pallas_call(
        functools.partial(finish_kernel, n, rows, tile, extra),
        grid=(1,),
        out_shape=(
            jax.ShapeDtypeStruct((n * rows, width), jnp.bfloat16),
            jax.ShapeDtypeStruct((1, width), jnp.float32),
        ),
        in_specs=specs,
        out_specs=(
            pl.BlockSpec((n * rows, width), lambda i: (0, 0)),
            pl.BlockSpec((1, width), lambda i: (0, 0)),
        ),
        scratch_shapes=[
            pltpu.VMEM((n * rows, width), jnp.float32),
            pltpu.VMEM((n, 8, width), jnp.float32),
        ],
        cost_estimate=pl.CostEstimate(
            flops=2 * elements * rank, bytes_accessed=8 * elements, transcendentals=0
        ),
    )(*args)


def merge(piece, low, high):
    return piece.astype(jnp.float32) + mix_rate * jnp.dot(
        low, high, preferred_element_type=jnp.float32
    )


def groups(full):
    wide = min(256, full)
    return [pl.ds(s, wide) for s in range(0, full, wide)]


def sums_kernel(weight_ref, low_ref, high_ref, sum_ref):
    @pl.when(pl.program_id(0) == 0)
    def _():
        sum_ref[...] = jnp.zeros_like(sum_ref)

    for at in groups(sum_ref.shape[1]):
        merged = merge(weight_ref[:, at], low_ref[...], high_ref[:, at])
        sum_ref[:, at] += jnp.sum(merged * merged, axis=0, keepdims=True)


def serve_kernel(weight_ref, low_ref, high_ref, column_ref, out_ref):
    for at in groups(out_ref.shape[1]):
        merged = merge(weight_ref[:, at], low_ref[...], high_ref[:, at])
        out_ref[:, at] = (merged * (1.0 / column_ref[:, at])).astype(out_ref.dtype)


def own_rows(kernel, weight, low, high, column, start, size):
    full, rank = weight.shape[1], high.shape[0]
    tile = min(size, 256)
    first = start // tile
    args = [weight, low, high]
    specs = [
        pl.BlockSpec((tile, full), lambda i: (first + i, 0)),
        pl.BlockSpec((tile, rank), lambda i: (first + i, 0)),
        pl.BlockSpec((rank, full), lambda i: (0, 0)),
    ]
    line = pl.BlockSpec((1, full), lambda i: (0, 0))
    if column is None:
        out_shape, out_spec = jax.ShapeDtypeStruct((1, full), jnp.float32), line
    else:
        args.append(column)
        specs.append(line)
        out_shape = jax.ShapeDtypeStruct((size, full), jnp.bfloat16)
        out_spec = pl.BlockSpec((tile, full), lambda i: (i, 0))
    return pl.pallas_call(
        kernel,
        grid=(size // tile,),
        out_shape=out_shape,
        in_specs=specs,
        out_specs=out_spec,
        cost_estimate=pl.CostEstimate(
            flops=2 * size * full * rank, bytes_accessed=4 * size * full, transcendentals=0
        ),
    )(*args)


def store_kernel(n, shift, rows, start, chunk_ref, _, out_ref, sem):
    owner = lax.rem(lax.axis_index("zero") + n - shift, n)
    at = pl.ds(pl.multiple_of(owner * rows + start, chunk_ref.shape[0]), chunk_ref.shape[0])
    copy = pltpu.make_async_copy(chunk_ref, out_ref.at[at], sem)
    copy.start()
    copy.wait()


def store_rows(n, shift, rows, start, chunk, whole):
    return pl.pallas_call(
        functools.partial(store_kernel, n, shift, rows, start),
        out_shape=jax.ShapeDtypeStruct(whole.shape, whole.dtype),
        in_specs=[pl.BlockSpec(memory_space=pltpu.VMEM), pl.BlockSpec(memory_space=pl.ANY)],
        out_specs=pl.BlockSpec(memory_space=pl.ANY),
        scratch_shapes=[pltpu.SemaphoreType.DMA],
        input_output_aliases={1: 0},
        compiler_params=pltpu.CompilerParams(vmem_limit_bytes=8 * 2**20),
        cost_estimate=pl.CostEstimate(flops=0, bytes_accessed=4 * chunk.size, transcendentals=0),
    )(chunk, whole)


def on_device(
    n,
    parts,
    weight_query,
    low_query,
    high_query,
    weight_key,
    low_key,
    high_key,
    weight_value,
    low_value,
    high_value,
    norm_train,
    norm_step,
):
    rows = weight_query.shape[0]
    rank = high_query.shape[0]
    me, tp = lax.axis_index("zero"), lax.axis_index("tp")

    def shifted(array):
        return [
            lax.ppermute(array, "zero", [(i, (i + k) % n) for i in range(n)])
            for k in range(1, n)
        ]

    def in_order(mine, others, axis):
        size = mine.shape[axis]
        shape = list(mine.shape)
        shape[axis] *= n
        whole = jnp.zeros(shape, mine.dtype)
        for slot, piece in enumerate([mine] + list(others)):
            at = [0] * len(shape)
            at[axis] = (me + n - slot) % n * size
            whole = lax.dynamic_update_slice(whole, piece, at)
        return whole

    value_parts = shifted(weight_value)

    piece = rows // parts
    lows = [
        lax.dynamic_slice(low, (tp * piece, 0), (piece, rank)).T
        for low in (low_key, low_value)
    ]
    norm = (norm_train + norm_step).astype(jnp.bfloat16)
    packed = jnp.concatenate(lows + [norm.reshape(-1, piece)], axis=0)
    shape = packed.shape
    if packed.size % 128 == 0:
        packed = packed.reshape(-1, 128)
    sent = shifted(packed)
    total = own_rows(sums_kernel, weight_query, low_query, high_query, None, 0, rows)
    totals = in_order(total, shifted(total), 0)
    column_query = jnp.sqrt(jnp.sum(totals, axis=0, keepdims=True))
    key_parts = shifted(weight_key)

    sizes = [rows // 2, rows // 4, rows // 8, rows // 16]
    sizes.append(rows - sum(sizes))
    mine, theirs, start = [], [], 0
    for size in sizes:
        chunk = own_rows(serve_kernel, weight_query, low_query, high_query, column_query, start, size)
        mine.append((start, chunk))
        theirs.append((start, shifted(chunk)))
        start += size

    packs = jnp.stack([a.reshape(shape) for a in [packed] + sent])
    packs = lax.all_gather(packs, "tp", axis=2, tiled=True)
    low_all = jnp.swapaxes(packs[:, : 2 * rank], 1, 2)
    gain = packs[:, 2 * rank :].reshape(n, -1, parts, piece)
    gain = jnp.swapaxes(gain, 1, 2).reshape(n, -1)
    serve_norm = in_order(gain[:1], [gain[k : k + 1] for k in range(1, n)], 0).reshape(-1)
    serve_value, column_value = finish(
        n, weight_value, value_parts, low_all[:, :, rank:], high_value, None
    )
    serve_key, column_key = finish(
        n, weight_key, key_parts, low_all[:, :, :rank], high_key, column_value
    )
    serve_query = jnp.zeros((n * rows, weight_query.shape[1]), jnp.bfloat16)
    for start, chunk in mine:
        serve_query = lax.dynamic_update_slice(serve_query, chunk, (me * rows + start, 0))
    for start, arrived in theirs:
        for k, chunk in enumerate(arrived):
            if start + chunk.shape[0] == rows:
                serve_query = store_rows(n, k + 1, rows, start, chunk, serve_query)
                continue
            owner = (me + n - 1 - k) % n
            serve_query = lax.dynamic_update_slice(serve_query, chunk, (owner * rows + start, 0))
    return (
        serve_query,
        serve_key,
        serve_value,
        column_query.reshape(-1),
        column_key.reshape(-1),
        column_value.reshape(-1),
        serve_norm,
    )


def solution(mesh):
    placed = (
        P(("unit", "zero"), "tp"),
        P(("unit", "zero"), None),
        P("unit", "tp"),
        P(("unit", "zero"), "tp"),
        P(("unit", "zero"), None),
        P("unit", "tp"),
        P(("unit", "zero"), "tp"),
        P(("unit", "zero"), None),
        P("unit", "tp"),
        P(("unit", "zero", "tp")),
        P(("unit", "zero", "tp")),
    )

    def body(*args):
        return on_device(mesh.shape["zero"], mesh.shape["tp"], *args)

    return jax.shard_map(
        body,
        mesh=mesh,
        in_specs=placed,
        out_specs=(
            P("unit", "tp"),
            P("unit", "tp"),
            P("unit", "tp"),
            P(("unit", "tp")),
            P(("unit", "tp")),
            P(("unit", "tp")),
            P("unit"),
        ),
        check_vma=False,
    )
```
